32 devices in a mesh: groups: 2 (over y), expert: 4 (over z), split: 2 (over x), pair: 2 (over core).
Axes of the slice: x: 2, y: 2, z: 4, core: 2. Of those that a mesh axis runs over, the one named last changes fastest.
Arguments:
- tokens: bfloat16 [64, 3584], P(('groups', 'expert'), ('split', 'pair')), parts along dimension 0, may hold values from -6 to 6
- routes: int32 [64, 2], P(('groups', 'expert')), parts along dimension 0, may hold values from 0 to 3, all different within a row; in each aligned block of 8 rows (0 to 7, 8 to 15, ...) at most 8 rows name the same one
- combine: float32 [64, 2], P(('groups', 'expert')), parts along dimension 0, may hold values from 0.05 to 1
- home: int32 [4], replicated, may hold values from 0 to 3, each once
- gate_up: bfloat16 [4, 3584, 2, 2560], P('expert', 'pair', None, 'split'), may hold values from -0.09375 to 0.09375
- down: bfloat16 [4, 2560, 3584], P('expert', ('split', 'pair')), may hold values from -0.15625 to 0.15625
Outputs:
- mixed: bfloat16 [64, 3584], P(('groups', 'expert'), ('split', 'pair')), parts along dimension 0
The draws below stay inside these ranges and needn't reach their ends.
There are 2 independent parts, one for each index of `groups`. The reference program is written for one: setup_inputs(seed, part) draws one part's arguments, and reference() takes and returns one part's arrays. A program takes and returns all parts, laid end to end along the dimension named above; an argument that names none is the same for every part. Nothing has to cross between parts.
Inputs may be any that keep to these rules, and one draw needn't show every extreme that they name: `routes`: each row names 2 different experts. In the rows of one device no expert is named more than 8 times, and some expert reaches 8 in every draw. A permutation: expert e is held in storage slot home[e].
All inputs are finite; a program needn't handle non-finite values.
Results may differ from the reference program's by a relative error of at most 0.025.
Values may be sent and summed in bfloat16 or wider, within the bound.
A program may use at most 64 MiB of HBM per device.

```python
import math
import jax
import jax.numpy as jnp
import numpy as np
from jax import lax

D = 3584
FF = 2560
TOK_DEV = 8
EXPERTS = 4
TOPK = 2
CAP = 8
TOKENS = 32
N_SPLIT = 2
N_PAIR = 2


def spiked(drawn, own_key, source, target, shards_of, factor):
    owner, partner = [(jnp.arange(drawn.shape[dim]) // (drawn.shape[dim] // shards_of)).reshape([-1 if axis == dim else 1 for axis in range(drawn.ndim)]) for dim in (source, target)]
    chosen = jax.random.permutation(own_key, shards_of)[partner]
    strong = (owner == chosen) | (owner == (partner + shards_of // 2) % shards_of)
    return jnp.where(strong, factor * drawn, drawn)


def levels(rng, shape, split, smallest, largest):
    factor_of, own = 1.0, jax.random.fold_in(rng, 6)
    for position, parts in split:
        steps = jnp.exp(jax.random.uniform(jax.random.fold_in(own, position), (parts,), jnp.float32, smallest / len(split), largest / len(split)))
        factor_of = factor_of * jnp.repeat(steps, shape[position] // parts).reshape([-1 if axis == position else 1 for axis in range(len(shape))])
    return factor_of


def shared_out(rng, own, number, rows, count, top, bound, lean):
    sequence = jax.random.permutation(rng, count)
    heavy_load, ordinary = load_shares(count, rows * top, bound, lean, True), load_shares(count, rows * top, bound, lean, False)
    places = jnp.arange(count)

    def named(tallies, offset_by):
        used = int((tallies > 0).sum())
        fixed = max(1, used // 4)
        passed = fixed + (places - fixed + offset_by * (used - fixed)) % max(1, count - fixed)
        return jnp.zeros((count,), jnp.int32).at[sequence[jnp.where(places < fixed, places, passed)]].set(jnp.asarray(tallies, jnp.int32))

    tallies = jnp.where(number % 4 == 0, named(heavy_load, number // 4), named(ordinary, number - number // 4 - 1))
    mixed = jax.random.permutation(jax.random.fold_in(own, 3), count)
    giver, receiver = mixed[0:count // 2 * 2:2], mixed[1:count // 2 * 2:2]
    room = jnp.minimum(tallies[giver] - 1, bound - tallies[receiver]) // 2
    room = jnp.where((giver == sequence[0]) | (receiver == sequence[0]) | (tallies[receiver] == 0), 0, jnp.maximum(room, 0))
    passed = jax.random.randint(jax.random.fold_in(own, 4), (count // 2,), 0, 1 << 20) % (room + 1)
    tallies = tallies.at[giver].add(-passed).at[receiver].add(passed)
    members = jnp.searchsorted(jnp.cumsum(tallies), jnp.arange(rows * top), side="right").astype(jnp.int32)
    listing = members.reshape(top, rows).T
    listing = listing[jax.random.permutation(jax.random.fold_in(own, 1), rows)]
    offset_by = jax.random.randint(jax.random.fold_in(own, 2), (rows, 1), 0, top)
    return jnp.take_along_axis(listing, (jnp.arange(top)[None, :] + offset_by) % top, axis=1)


def load_shares(number_of, total, most, lean, full):
    portions = [(1 << 20) // math.isqrt(rank ** lean) + 1 for rank in range(1, number_of + 1)]
    largest = most if full else min(most, max(-(-total // number_of), total * portions[0] // sum(portions)))
    least = 1 if total - largest >= number_of - 1 else 0
    holding, rest = [largest] + [least] * (number_of - 1), total - largest - least * (number_of - 1)
    while rest > 0:
        movable = [i for i in range(1, number_of) if holding[i] < largest] or [i for i in range(1, number_of) if holding[i] < most]
        pool, left = sum([portions[i] for i in movable]), rest
        for i in movable:
            addition = min(most - holding[i], max(1, left * portions[i] // pool), rest)
            holding[i] = holding[i] + addition
            rest = rest - addition
    return np.array(holding)


def centred(key, shape, spread, bound, cuts=(), held_as=jnp.bfloat16):
    result = jax.random.normal(key, shape, jnp.float32) * spread
    if len(cuts) > 0:
        result = levels(key, shape, cuts, -0.22, 0.18) * result
    return jnp.clip(result, min=-bound, max=bound).astype(held_as)


def gaussian_with(own_key, shape, spread, limit, split, heavy, held_as=jnp.bfloat16):
    array = spread * jax.random.normal(own_key, shape, jnp.float32)
    if split:
        array = array * levels(own_key, shape, split, -0.22, 0.18)
    return jnp.clip(spiked(array, jax.random.fold_in(own_key, 3), *heavy), -limit, limit).astype(held_as)


def setup_inputs(seed: int = 0, part: int = 0) -> dict:
    keys = jax.random.split(jax.random.key(seed), 7)
    part_keys = jax.random.split(jax.random.fold_in(keys[6], part), 7)
    tokens = centred(part_keys[0], (TOKENS, D), 1.0, 6.0, ((0, 4), (1, 4)))
    routes_keys = jax.random.split(jax.random.fold_in(part_keys[1], 1), TOKENS // TOK_DEV)
    routes_turns = jax.random.permutation(jax.random.fold_in(part_keys[1], 3), TOKENS // TOK_DEV)
    routes = jax.vmap(lambda own, number: shared_out(jax.random.fold_in(part_keys[1], 2), own, number, TOK_DEV, EXPERTS, TOPK, CAP, 2))(routes_keys, routes_turns).reshape((TOKENS, TOPK))
    combine = jnp.clip(jnp.exp(math.log(1.0) - 2.9957323 * jax.random.uniform(part_keys[2], (TOKENS, TOPK), jnp.float32) ** levels(part_keys[2], (TOKENS, TOPK), ((0, 4),), -0.2, 0.2)), 0.05, 1.0)
    home = jax.random.permutation(keys[3], EXPERTS).astype(jnp.int32)
    gate_up = centred(keys[4], (EXPERTS, D, 2, FF), D ** -0.5, 0.09375, ((0, 4), (1, 2), (3, 2)))
    down = gaussian_with(keys[5], (EXPERTS, FF, D), FF ** -0.5, 0.15625, ((0, 4), (1, 4)), (1, 2, 4, 2.0))
    return dict(tokens=tokens, routes=routes, combine=combine, home=home, gate_up=gate_up, down=down)


def reference(tokens, routes, combine, home, gate_up, down):
    count = tokens.shape[0]
    blocks = N_SPLIT * N_PAIR
    block_width = FF // blocks
    slot = home[routes].astype(jnp.int32)

    def one_expert(index):
        weights = gate_up[index]
        gate = jnp.dot(tokens, weights[:, 0, :], preferred_element_type=jnp.float32)
        upward = jnp.dot(tokens, weights[:, 1, :], preferred_element_type=jnp.float32)
        hidden = (jax.nn.silu(gate) * upward).astype(jnp.bfloat16)
        pieces = hidden.reshape(count, blocks, block_width).astype(jnp.float32)
        down_blocks = down[index].reshape(blocks, block_width, D).astype(jnp.float32)
        partial_value = jnp.einsum('tbw,bwd->btd', pieces, down_blocks).astype(jnp.bfloat16)
        partial_value = lax.optimization_barrier(partial_value)
        return jnp.sum(partial_value.astype(jnp.float32), axis=0).astype(jnp.bfloat16)

    outputs = lax.map(one_expert, jnp.arange(EXPERTS, dtype=jnp.int32))
    chosen = (slot[:, :, None] == jnp.arange(EXPERTS, dtype=jnp.int32)[None, None, :])
    mixing = jnp.sum(jnp.where(chosen, combine[:, :, None], jnp.float32(0.0)), axis=1)
    mixed = jnp.einsum('ts,std->td', mixing, outputs.astype(jnp.float32), precision=lax.Precision.HIGHEST)
    return mixed.astype(jnp.bfloat16)
```

```python
import functools
import jax
import jax.numpy as jnp
from jax import lax
from jax.experimental import pallas as pl
from jax.experimental.pallas import tpu as pltpu
from jax.sharding import PartitionSpec as P

MESH = pl.DeviceIdType.MESH
LANES = 128


def fused(
    n_expert, chunks,
    tokens_hbm, routes_ref, combine_ref, home_ref, gate_up_hbm, down_hbm, out_ref,
    own, tok, spread, xi, wbuf, dbuf, mine, pre_out, pre_in, part_out, part_in, kept, stage, fin, mixbuf,
    load_sem, w_sem, d_sem, tok_send, tok_recv, pre_send, pre_recv, part_send, part_recv, fin_send, fin_recv,
):
    groups, expert = lax.axis_index("groups"), lax.axis_index("expert")
    split, pair = lax.axis_index("split"), lax.axis_index("pair")
    partner = (groups, expert, split, 1 - pair)
    rows, narrow = tokens_hbm.shape
    depth = gate_up_hbm.shape[1]
    half = gate_up_hbm.shape[3] // 2
    blocks = half // LANES
    all_rows = n_expert * rows

    load = pltpu.make_async_copy(tokens_hbm, own, load_sem)
    load.start()
    step = depth // chunks
    w_loads = []
    for h in range(2):
        at = pl.multiple_of(lax.rem(1 - pair + h, 2) * half, LANES)
        for c in range(chunks):
            w_loads.append(pltpu.make_async_copy(
                gate_up_hbm.at[0, pl.ds(c * step, step), :, pl.ds(at, half)],
                wbuf.at[h, pl.ds(c * step, step)], w_sem.at[h, c]))
            w_loads[-1].start()
    d_loads = []
    for h in range(2):
        core = lax.rem(1 - pair + h, 2)
        for s in range(2):
            at = pl.multiple_of((2 * s + core) * narrow, LANES)
            d_loads.append(pltpu.make_async_copy(
                down_hbm.at[0, :, pl.ds(at, narrow)],
                dbuf.at[h, :, pl.ds(s * narrow, narrow)], d_sem.at[h, s]))
            d_loads[-1].start()

    barrier = pltpu.get_barrier_semaphore()
    for de in range(n_expert):
        for ds in range(2):
            for dp in range(2):
                if de + ds + dp:
                    pl.semaphore_signal(barrier, inc=1, device_id=(
                        groups, lax.rem(expert + de, n_expert), lax.rem(split + ds, 2), lax.rem(pair + dp, 2)),
                        device_id_type=MESH)

    experts_all = home_ref.shape[0]
    chosen_count = routes_ref.shape[0]
    square = (rows, rows)
    diagonal = lax.broadcasted_iota(jnp.int32, square, 0) == lax.broadcasted_iota(jnp.int32, square, 1)
    slot_rows = jnp.zeros((chosen_count, rows), jnp.int32)
    for e in range(experts_all):
        slot_rows = jnp.where(routes_ref[...] == e, home_ref[e], slot_rows)
    for e in range(n_expert):
        weight = jnp.sum(jnp.where(slot_rows == e, combine_ref[...], 0.0), axis=0, keepdims=True)
        column = jnp.sum(jnp.where(diagonal, jnp.broadcast_to(weight, square), 0.0), axis=1, keepdims=True)
        mixbuf[e] = jnp.broadcast_to(column, (rows, LANES))
    shape = (LANES, 4 * LANES)
    source = lax.broadcasted_iota(jnp.int32, shape, 0)
    place = lax.broadcasted_iota(jnp.int32, shape, 1)
    wanted = jnp.where(place < 2 * LANES, 2 * source, 2 * source + 2 * LANES + 1)
    spread[...] = jnp.where(place == wanted, 1.0, 0.0).astype(jnp.bfloat16)

    load.wait()
    pl.semaphore_wait(barrier, 4 * n_expert - 1)

    def tok_copy(de, ds):
        return pltpu.make_async_remote_copy(
            src_ref=own, dst_ref=tok.at[de, pair], send_sem=tok_send.at[de, ds], recv_sem=tok_recv.at[de, pair],
            device_id=(groups, lax.rem(expert + de, n_expert), lax.rem(split + ds, 2), split), device_id_type=MESH)

    local = pltpu.make_async_copy(own, tok.at[0, pair], tok_recv.at[0, pair])
    order = sorted(range(n_expert), key=lambda de: -min(de, n_expert - de))
    for de in order:
        for ds in (1, 0):
            if de or ds:
                tok_copy(de, ds).start()

    @pl.when(pair == split)
    def _():
        local.start()

    @pl.when(pair != split)
    def _():
        tok_copy(0, 0).start()

    for w_load in w_loads:
        w_load.wait()
    for de in range(n_expert):
        for h in range(2):
            pltpu.make_async_copy(own, tok.at[de, h], tok_recv.at[de, h]).wait()

    pieces = []
    for h in range(2):
        whole = jnp.concatenate([tok[de, h].astype(jnp.float32) for de in range(n_expert)], axis=0)
        for c in range(narrow // LANES):
            pieces.append(whole[:, c * LANES:(c + 1) * LANES])
    stacked = jnp.concatenate(pieces, axis=0).astype(jnp.bfloat16)
    wide = jnp.dot(stacked, spread[...], preferred_element_type=jnp.float32).astype(jnp.bfloat16)
    for c in range(len(pieces)):
        at = c * 2 * LANES
        xi[0:all_rows, at:at + 2 * LANES] = wide[c * all_rows:(c + 1) * all_rows, 0:2 * LANES]
        xi[all_rows:, at:at + 2 * LANES] = wide[c * all_rows:(c + 1) * all_rows, 2 * LANES:]

    def weights(number):
        h, j = number // blocks, number % blocks
        return wbuf[h, :, :, j * LANES:(j + 1) * LANES].reshape(2 * depth, LANES)

    def pre_copy(k):
        at = (0, 2 * (blocks // 2) * LANES, half)
        cols = pl.ds(at[k], at[k + 1] - at[k])
        return pltpu.make_async_remote_copy(
            src_ref=pre_out.at[:, cols], dst_ref=pre_in.at[:, cols], send_sem=pre_send.at[k],
            recv_sem=pre_recv.at[k], device_id=partner, device_id_type=MESH)

    pre_copies = [pre_copy(0)] + ([pre_copy(1)] if blocks % 2 else [])
    for n in range(blocks):
        numbers = (2 * n, 2 * n + 1)
        w = jnp.concatenate([weights(k) for k in numbers], axis=1)
        value = jnp.dot(xi[...], w, preferred_element_type=jnp.float32)
        for i, k in enumerate(numbers):
            piece = value[:, i * LANES:(i + 1) * LANES]
            if k < blocks:
                pre_out[:, k * LANES:(k + 1) * LANES] = piece.astype(jnp.bfloat16)
            else:
                mine[:, (k - blocks) * LANES:(k - blocks + 1) * LANES] = piece
        if n == blocks // 2 - 1:
            pre_copies[0].start()
        if blocks % 2 and n == blocks // 2:
            pre_copies[1].start()

    for copy in pre_copies:
        copy.wait_recv()
    total = mine[...] + pre_in[...].astype(jnp.float32)
    gate, up = total[0:all_rows], total[all_rows:]
    hidden = (gate / (1.0 + jnp.exp(-gate)) * up).astype(jnp.bfloat16)

    for d_load in d_loads:
        d_load.wait()
    part_out[...] = jnp.dot(hidden, dbuf[0], preferred_element_type=jnp.float32).astype(jnp.bfloat16)
    part = pltpu.make_async_remote_copy(
        src_ref=part_out, dst_ref=part_in, send_sem=part_send, recv_sem=part_recv,
        device_id=partner, device_id_type=MESH)
    part.start()
    kept[...] = jnp.dot(hidden, dbuf[1], preferred_element_type=jnp.float32)
    part.wait_recv()

    def fin_copy(de, ds):
        return pltpu.make_async_remote_copy(
            src_ref=stage.at[lax.rem(split + ds, 2), de], dst_ref=fin.at[de, ds],
            send_sem=fin_send.at[de, ds], recv_sem=fin_recv.at[de, ds],
            device_id=(groups, lax.rem(expert + de, n_expert), lax.rem(split + ds, 2), pair), device_id_type=MESH)

    for de in order:
        block = (n_expert - de) % n_expert
        for s in range(2):
            at = slice(s * narrow, (s + 1) * narrow)
            lines = slice(block * rows, (block + 1) * rows)
            stage[s, de] = (kept[lines, at] + part_in[:, at].astype(jnp.float32)[lines]).astype(jnp.bfloat16)
        for ds in (1, 0):
            if de or ds:
                fin_copy(de, ds).start()

    result = jnp.zeros((rows, narrow), jnp.float32)
    for de in reversed(order):
        source = lax.rem(expert + n_expert - de, n_expert)
        pair_sum = jnp.zeros((rows, narrow), jnp.float32)
        for ds in range(2):
            if de or ds:
                fin_copy(de, ds).wait_recv()
                pair_sum += fin[de, ds].astype(jnp.float32)
            else:
                pair_sum += stage[split, 0].astype(jnp.float32)
        result += mixbuf[source][:, 0:1] * pair_sum
    out_ref[...] = result.astype(out_ref.dtype)

    for de in range(n_expert):
        for ds in range(2):
            if de or ds:
                tok_copy(de, ds).wait_send()
                fin_copy(de, ds).wait_send()

    @pl.when(pair != split)
    def _():
        tok_copy(0, 0).wait_send()

    for copy in pre_copies:
        copy.wait_send()
    part.wait_send()


def fused_shards(tokens, routes, combine, home, gate_up, down):
    n_expert = lax.axis_size("expert")
    rows, narrow = tokens.shape
    depth, width = gate_up.shape[1], gate_up.shape[3]
    half = width // 2
    all_rows = n_expert * rows
    bf16, f32 = jnp.bfloat16, jnp.float32
    chunks = 4 if depth % 64 == 0 else 1
    vmem, anywhere = pl.BlockSpec(memory_space=pltpu.VMEM), pl.BlockSpec(memory_space=pl.ANY)
    dma = pltpu.SemaphoreType.DMA
    return pl.pallas_call(
        functools.partial(fused, n_expert, chunks),
        out_shape=jax.ShapeDtypeStruct((rows, narrow), bf16),
        in_specs=[anywhere, vmem, vmem, pl.BlockSpec(memory_space=pltpu.SMEM), anywhere, anywhere],
        out_specs=vmem,
        scratch_shapes=[
            pltpu.VMEM((rows, narrow), bf16),
            pltpu.VMEM((n_expert, 2, rows, narrow), bf16),
            pltpu.VMEM((LANES, 4 * LANES), bf16),
            pltpu.VMEM((2 * all_rows, 2 * depth), bf16),
            pltpu.VMEM((2, depth, 2, half), bf16),
            pltpu.VMEM((2, down.shape[1], 2 * narrow), bf16),
            pltpu.VMEM((2 * all_rows, half), f32),
            pltpu.VMEM((2 * all_rows, half), bf16),
            pltpu.VMEM((2 * all_rows, half), bf16),
            pltpu.VMEM((all_rows, 2 * narrow), bf16),
            pltpu.VMEM((all_rows, 2 * narrow), bf16),
            pltpu.VMEM((all_rows, 2 * narrow), f32),
            pltpu.VMEM((2, n_expert, rows, narrow), bf16),
            pltpu.VMEM((n_expert, 2, rows, narrow), bf16),
            pltpu.VMEM((n_expert, rows, LANES), f32),
            dma, dma((2, chunks)), dma((2, 2)),
            dma((n_expert, 2)), dma((n_expert, 2)), dma((2,)), dma((2,)), dma, dma,
            dma((n_expert, 2)), dma((n_expert, 2)),
        ],
        compiler_params=pltpu.CompilerParams(
            collective_id=0, has_side_effects=True, vmem_limit_bytes=40 * 2**20),
    )(tokens, routes.T, combine.T, home, gate_up, down)


def fits(mesh):
    return mesh.shape["split"] == 2 and mesh.shape["pair"] == 2


def placed_body(mesh):
    def body(tokens, routes, combine, home, gate_up, down):
        aligned = (
            tokens.shape[0] == 8 and tokens.shape[1] % LANES == 0 and gate_up.shape[0] == 1
            and gate_up.shape[3] % (2 * LANES) == 0 and home.shape[0] == mesh.shape["expert"]
        )
        chosen = fused_shards if fits(mesh) and aligned else shards
        return chosen(tokens, routes, combine, home, gate_up, down)

    return body


def shards(tokens, routes, combine, home, gate_up, down):
    n_expert = lax.axis_size("expert")
    local_tokens = tokens.shape[0]
    chosen_count = routes.shape[1]
    experts_all = home.shape[0]
    experts_here = gate_up.shape[0]
    total_rows = experts_all * local_tokens
    width = gate_up.shape[1] * 2
    table_ids = jnp.arange(experts_all, dtype=jnp.int32)
    slot = jnp.sum(
        jnp.where(routes[:, :, None] == table_ids[None, None, :], home[None, None, :], 0), axis=-1
    )
    flat_slot = slot.reshape(-1)
    entries = flat_slot.shape[0]
    order_ids = jnp.arange(entries, dtype=jnp.int32)
    earlier = (flat_slot[:, None] == flat_slot[None, :]) & (order_ids[None, :] < order_ids[:, None])
    position = jnp.sum(earlier.astype(jnp.int32), axis=1)
    target = (flat_slot * local_tokens + position).reshape(local_tokens, chosen_count)
    row_ids = jnp.arange(total_rows, dtype=jnp.int32)
    hits = target[None, :, :] == row_ids[:, None, None]
    placing = jnp.sum(hits.astype(jnp.int32), axis=-1).astype(jnp.bfloat16)
    mixing = jnp.sum(jnp.where(hits, combine[None, :, :], jnp.float32(0.0)), axis=-1).T
    outgoing = jnp.dot(placing, tokens, preferred_element_type=jnp.float32).astype(jnp.bfloat16)
    arrived = lax.all_to_all(outgoing, "expert", split_axis=0, concat_axis=0, tiled=True)
    gathered = lax.all_gather(arrived, ("split", "pair"), axis=1, tiled=True)
    rows_each = n_expert * local_tokens
    inputs = gathered.reshape(n_expert, experts_here, local_tokens, width)
    inputs = jnp.swapaxes(inputs, 0, 1).reshape(experts_here, rows_each, width)
    pair_index = lax.axis_index("pair")
    half_width = gate_up.shape[1]
    own_half = lax.dynamic_slice_in_dim(inputs, pair_index * half_width, half_width, 2)
    before = jnp.einsum("erd,edgf->ergf", own_half, gate_up, preferred_element_type=jnp.float32)
    before = lax.psum_scatter(
        before.astype(jnp.bfloat16), "pair", scatter_dimension=3, tiled=True
    ).astype(jnp.float32)
    hidden = (jax.nn.silu(before[:, :, 0, :]) * before[:, :, 1, :]).astype(jnp.bfloat16)
    partial_value = jnp.einsum(
        "erf,efd->erd", hidden, down, preferred_element_type=jnp.float32
    ).astype(jnp.bfloat16)
    summed = (
        lax.psum_scatter(partial_value, ("split", "pair"), scatter_dimension=2, tiled=True)
        .astype(jnp.float32)
        .astype(jnp.bfloat16)
    )
    narrow = summed.shape[2]
    returning = jnp.swapaxes(summed.reshape(experts_here, n_expert, local_tokens, narrow), 0, 1)
    returning = returning.reshape(total_rows, narrow)
    results = lax.all_to_all(returning, "expert", split_axis=0, concat_axis=0, tiled=True)
    mixed = jnp.dot(mixing, results.astype(jnp.float32), precision=lax.Precision.HIGHEST)
    return mixed.astype(jnp.bfloat16)


def solution(mesh):
    placed = (
        P(("groups", "expert"), ("split", "pair")),
        P(("groups", "expert"), None),
        P(("groups", "expert"), None),
        P(),
        P("expert", "pair", None, "split"),
        P("expert", ("split", "pair"), None),
    )
    return jax.shard_map(
        placed_body(mesh),
        mesh=mesh,
        in_specs=placed,
        out_specs=P(("groups", "expert"), ("split", "pair")),
        check_vma=False,
    )
```

```python
import functools
import jax
import jax.numpy as jnp
from jax import lax
from jax.experimental import pallas as pl
from jax.experimental.pallas import tpu as pltpu
from jax.sharding import PartitionSpec as P

MESH = pl.DeviceIdType.MESH
LANES = 128


def fused(
    n_expert, chunks,
    tokens_hbm, routes_hbm, combine_hbm, home_hbm, gate_up_hbm, down_hbm, out_ref,
    routes_ref, combine_ref, home_ref, own, tok, spread, xi, wbuf, dbuf, mine, pre_out, pre_in, part_out, part_in, kept, stage, fin, mixbuf,
    load_sem, w_sem, d_sem, tok_send, tok_recv, pre_send, pre_recv, part_send, part_recv, fin_send, fin_recv,
):
    groups, expert = lax.axis_index("groups"), lax.axis_index("expert")
    split, pair = lax.axis_index("split"), lax.axis_index("pair")
    partner = (groups, expert, split, 1 - pair)
    rows, narrow = tokens_hbm.shape
    depth = gate_up_hbm.shape[1]
    half = gate_up_hbm.shape[3] // 2
    blocks = half // LANES
    all_rows = n_expert * rows

    load = pltpu.make_async_copy(tokens_hbm, own, load_sem.at[0])
    load.start()
    tables = [
        pltpu.make_async_copy(routes_hbm, routes_ref, load_sem.at[1]),
        pltpu.make_async_copy(combine_hbm, combine_ref, load_sem.at[2]),
        pltpu.make_async_copy(home_hbm, home_ref, load_sem.at[3]),
    ]
    for table in tables:
        table.start()
    step = depth // chunks
    w_loads = []
    for h in range(2):
        at = pl.multiple_of(lax.rem(1 - pair + h, 2) * half, LANES)
        for c in range(chunks):
            w_loads.append(pltpu.make_async_copy(
                gate_up_hbm.at[0, pl.ds(c * step, step), :, pl.ds(at, half)],
                wbuf.at[h, pl.ds(c * step, step)], w_sem.at[h, c]))
            w_loads[-1].start()
    d_loads = []
    for h in range(2):
        core = lax.rem(1 - pair + h, 2)
        for s in range(2):
            at = pl.multiple_of((2 * s + core) * narrow, LANES)
            d_loads.append(pltpu.make_async_copy(
                down_hbm.at[0, :, pl.ds(at, narrow)],
                dbuf.at[h, :, pl.ds(s * narrow, narrow)], d_sem.at[h, s]))
            d_loads[-1].start()

    barrier = pltpu.get_barrier_semaphore()
    for de in range(n_expert):
        for ds in range(2):
            for dp in range(2):
                if de + ds + dp:
                    pl.semaphore_signal(barrier, inc=1, device_id=(
                        groups, lax.rem(expert + de, n_expert), lax.rem(split + ds, 2), lax.rem(pair + dp, 2)),
                        device_id_type=MESH)

    load.wait()
    pl.semaphore_wait(barrier, 4 * n_expert - 1)

    def tok_copy(de, ds):
        return pltpu.make_async_remote_copy(
            src_ref=own, dst_ref=tok.at[de, pair], send_sem=tok_send.at[de, ds], recv_sem=tok_recv.at[de, pair],
            device_id=(groups, lax.rem(expert + de, n_expert), lax.rem(split + ds, 2), split), device_id_type=MESH)

    local = pltpu.make_async_copy(own, tok.at[0, pair], tok_recv.at[0, pair])
    order = sorted(range(n_expert), key=lambda de: -min(de, n_expert - de))
    for de in order:
        for ds in (1, 0):
            if de or ds:
                tok_copy(de, ds).start()

    @pl.when(pair == split)
    def _():
        local.start()

    @pl.when(pair != split)
    def _():
        tok_copy(0, 0).start()

    for table in tables:
        table.wait()
    experts_all = home_ref.shape[0]
    chosen_count = routes_ref.shape[0]
    square = (rows, rows)
    diagonal = lax.broadcasted_iota(jnp.int32, square, 0) == lax.broadcasted_iota(jnp.int32, square, 1)
    slot_rows = jnp.zeros((chosen_count, rows), jnp.int32)
    for e in range(experts_all):
        slot_rows = jnp.where(routes_ref[...] == e, home_ref[e], slot_rows)
    for e in range(n_expert):
        weight = jnp.sum(jnp.where(slot_rows == e, combine_ref[...], 0.0), axis=0, keepdims=True)
        column = jnp.sum(jnp.where(diagonal, jnp.broadcast_to(weight, square), 0.0), axis=1, keepdims=True)
        mixbuf[e] = jnp.broadcast_to(column, (rows, LANES))
    shape = (LANES, 4 * LANES)
    source = lax.broadcasted_iota(jnp.int32, shape, 0)
    place = lax.broadcasted_iota(jnp.int32, shape, 1)
    wanted = jnp.where(place < 2 * LANES, 2 * source, 2 * source + 2 * LANES + 1)
    spread[...] = jnp.where(place == wanted, 1.0, 0.0).astype(jnp.bfloat16)

    for w_load in w_loads:
        w_load.wait()
    for de in range(n_expert):
        for h in range(2):
            pltpu.make_async_copy(own, tok.at[de, h], tok_recv.at[de, h]).wait()

    pieces = []
    for h in range(2):
        whole = jnp.concatenate([tok[de, h].astype(jnp.float32) for de in range(n_expert)], axis=0)
        for c in range(narrow // LANES):
            pieces.append(whole[:, c * LANES:(c + 1) * LANES])
    stacked = jnp.concatenate(pieces, axis=0).astype(jnp.bfloat16)
    wide = jnp.dot(stacked, spread[...], preferred_element_type=jnp.float32).astype(jnp.bfloat16)
    for c in range(len(pieces)):
        at = c * 2 * LANES
        xi[0:all_rows, at:at + 2 * LANES] = wide[c * all_rows:(c + 1) * all_rows, 0:2 * LANES]
        xi[all_rows:, at:at + 2 * LANES] = wide[c * all_rows:(c + 1) * all_rows, 2 * LANES:]

    def weights(number):
        h, j = number // blocks, number % blocks
        return wbuf[h, :, :, j * LANES:(j + 1) * LANES].reshape(2 * depth, LANES)

    def pre_copy(k):
        at = (0, 2 * (blocks // 2) * LANES, half)
        cols = pl.ds(at[k], at[k + 1] - at[k])
        return pltpu.make_async_remote_copy(
            src_ref=pre_out.at[:, cols], dst_ref=pre_in.at[:, cols], send_sem=pre_send.at[k],
            recv_sem=pre_recv.at[k], device_id=partner, device_id_type=MESH)

    pre_copies = [pre_copy(0)] + ([pre_copy(1)] if blocks % 2 else [])
    for n in range(blocks):
        numbers = (2 * n, 2 * n + 1)
        w = jnp.concatenate([weights(k) for k in numbers], axis=1)
        value = jnp.dot(xi[...], w, preferred_element_type=jnp.float32)
        for i, k in enumerate(numbers):
            piece = value[:, i * LANES:(i + 1) * LANES]
            if k < blocks:
                pre_out[:, k * LANES:(k + 1) * LANES] = piece.astype(jnp.bfloat16)
            else:
                mine[:, (k - blocks) * LANES:(k - blocks + 1) * LANES] = piece
        if n == blocks // 2 - 1:
            pre_copies[0].start()
        if blocks % 2 and n == blocks // 2:
            pre_copies[1].start()

    for copy in pre_copies:
        copy.wait_recv()
    total = mine[...] + pre_in[...].astype(jnp.float32)
    gate, up = total[0:all_rows], total[all_rows:]
    hidden = (gate / (1.0 + jnp.exp(-gate)) * up).astype(jnp.bfloat16)

    for d_load in d_loads:
        d_load.wait()
    part_out[...] = jnp.dot(hidden, dbuf[0], preferred_element_type=jnp.float32).astype(jnp.bfloat16)
    part = pltpu.make_async_remote_copy(
        src_ref=part_out, dst_ref=part_in, send_sem=part_send, recv_sem=part_recv,
        device_id=partner, device_id_type=MESH)
    part.start()
    kept[...] = jnp.dot(hidden, dbuf[1], preferred_element_type=jnp.float32)
    part.wait_recv()

    def fin_copy(de, ds):
        return pltpu.make_async_remote_copy(
            src_ref=stage.at[lax.rem(split + ds, 2), de], dst_ref=fin.at[de, ds],
            send_sem=fin_send.at[de, ds], recv_sem=fin_recv.at[de, ds],
            device_id=(groups, lax.rem(expert + de, n_expert), lax.rem(split + ds, 2), pair), device_id_type=MESH)

    for de in order:
        block = (n_expert - de) % n_expert
        for s in range(2):
            at = slice(s * narrow, (s + 1) * narrow)
            lines = slice(block * rows, (block + 1) * rows)
            stage[s, de] = (kept[lines, at] + part_in[:, at].astype(jnp.float32)[lines]).astype(jnp.bfloat16)
        for ds in (1, 0):
            if de or ds:
                fin_copy(de, ds).start()

    result = jnp.zeros((rows, narrow), jnp.float32)
    for de in reversed(order):
        source = lax.rem(expert + n_expert - de, n_expert)
        pair_sum = jnp.zeros((rows, narrow), jnp.float32)
        for ds in range(2):
            if de or ds:
                fin_copy(de, ds).wait_recv()
                pair_sum += fin[de, ds].astype(jnp.float32)
            else:
                pair_sum += stage[split, 0].astype(jnp.float32)
        result += mixbuf[source][:, 0:1] * pair_sum
    out_ref[...] = result.astype(out_ref.dtype)

    for de in range(n_expert):
        for ds in range(2):
            if de or ds:
                tok_copy(de, ds).wait_send()
                fin_copy(de, ds).wait_send()

    @pl.when(pair != split)
    def _():
        tok_copy(0, 0).wait_send()

    for copy in pre_copies:
        copy.wait_send()
    part.wait_send()


def fused_shards(tokens, routes, combine, home, gate_up, down):
    n_expert = lax.axis_size("expert")
    rows, narrow = tokens.shape
    depth, width = gate_up.shape[1], gate_up.shape[3]
    half = width // 2
    all_rows = n_expert * rows
    bf16, f32 = jnp.bfloat16, jnp.float32
    chunks = 4 if depth % 64 == 0 else 1
    in_hbm = pl.BlockSpec(memory_space=pltpu.HBM)
    dma = pltpu.SemaphoreType.DMA
    return pl.pallas_call(
        functools.partial(fused, n_expert, chunks),
        out_shape=jax.ShapeDtypeStruct((rows, narrow), bf16),
        in_specs=[in_hbm] * 6,
        out_specs=pl.BlockSpec(memory_space=pltpu.VMEM),
        scratch_shapes=[
            pltpu.VMEM(routes.shape[::-1], jnp.int32),
            pltpu.VMEM(combine.shape[::-1], f32),
            pltpu.SMEM(home.shape, jnp.int32),
            pltpu.VMEM((rows, narrow), bf16),
            pltpu.VMEM((n_expert, 2, rows, narrow), bf16),
            pltpu.VMEM((LANES, 4 * LANES), bf16),
            pltpu.VMEM((2 * all_rows, 2 * depth), bf16),
            pltpu.VMEM((2, depth, 2, half), bf16),
            pltpu.VMEM((2, down.shape[1], 2 * narrow), bf16),
            pltpu.VMEM((2 * all_rows, half), f32),
            pltpu.VMEM((2 * all_rows, half), bf16),
            pltpu.VMEM((2 * all_rows, half), bf16),
            pltpu.VMEM((all_rows, 2 * narrow), bf16),
            pltpu.VMEM((all_rows, 2 * narrow), bf16),
            pltpu.VMEM((all_rows, 2 * narrow), f32),
            pltpu.VMEM((2, n_expert, rows, narrow), bf16),
            pltpu.VMEM((n_expert, 2, rows, narrow), bf16),
            pltpu.VMEM((n_expert, rows, LANES), f32),
            dma((4,)), dma((2, chunks)), dma((2, 2)),
            dma((n_expert, 2)), dma((n_expert, 2)), dma((2,)), dma((2,)), dma, dma,
            dma((n_expert, 2)), dma((n_expert, 2)),
        ],
        compiler_params=pltpu.CompilerParams(
            collective_id=0, has_side_effects=True, vmem_limit_bytes=67_043_328),
    )(tokens, routes.T, combine.T, home, gate_up, down)


def fits(mesh):
    return mesh.shape["split"] == 2 and mesh.shape["pair"] == 2


def placed_body(mesh):
    def body(tokens, routes, combine, home, gate_up, down):
        aligned = (
            tokens.shape[0] == 8 and tokens.shape[1] % LANES == 0 and gate_up.shape[0] == 1
            and gate_up.shape[3] % (2 * LANES) == 0 and home.shape[0] == mesh.shape["expert"]
        )
        chosen = fused_shards if fits(mesh) and aligned else shards
        return chosen(tokens, routes, combine, home, gate_up, down)

    return body


def shards(tokens, routes, combine, home, gate_up, down):
    n_expert = lax.axis_size("expert")
    local_tokens = tokens.shape[0]
    chosen_count = routes.shape[1]
    experts_all = home.shape[0]
    experts_here = gate_up.shape[0]
    total_rows = experts_all * local_tokens
    width = gate_up.shape[1] * 2
    table_ids = jnp.arange(experts_all, dtype=jnp.int32)
    slot = jnp.sum(
        jnp.where(routes[:, :, None] == table_ids[None, None, :], home[None, None, :], 0), axis=-1
    )
    flat_slot = slot.reshape(-1)
    entries = flat_slot.shape[0]
    order_ids = jnp.arange(entries, dtype=jnp.int32)
    earlier = (flat_slot[:, None] == flat_slot[None, :]) & (order_ids[None, :] < order_ids[:, None])
    position = jnp.sum(earlier.astype(jnp.int32), axis=1)
    target = (flat_slot * local_tokens + position).reshape(local_tokens, chosen_count)
    row_ids = jnp.arange(total_rows, dtype=jnp.int32)
    hits = target[None, :, :] == row_ids[:, None, None]
    placing = jnp.sum(hits.astype(jnp.int32), axis=-1).astype(jnp.bfloat16)
    mixing = jnp.sum(jnp.where(hits, combine[None, :, :], jnp.float32(0.0)), axis=-1).T
    outgoing = jnp.dot(placing, tokens, preferred_element_type=jnp.float32).astype(jnp.bfloat16)
    arrived = lax.all_to_all(outgoing, "expert", split_axis=0, concat_axis=0, tiled=True)
    gathered = lax.all_gather(arrived, ("split", "pair"), axis=1, tiled=True)
    rows_each = n_expert * local_tokens
    inputs = gathered.reshape(n_expert, experts_here, local_tokens, width)
    inputs = jnp.swapaxes(inputs, 0, 1).reshape(experts_here, rows_each, width)
    pair_index = lax.axis_index("pair")
    half_width = gate_up.shape[1]
    own_half = lax.dynamic_slice_in_dim(inputs, pair_index * half_width, half_width, 2)
    before = jnp.einsum("erd,edgf->ergf", own_half, gate_up, preferred_element_type=jnp.float32)
    before = lax.psum_scatter(
        before.astype(jnp.bfloat16), "pair", scatter_dimension=3, tiled=True
    ).astype(jnp.float32)
    hidden = (jax.nn.silu(before[:, :, 0, :]) * before[:, :, 1, :]).astype(jnp.bfloat16)
    partial_value = jnp.einsum(
        "erf,efd->erd", hidden, down, preferred_element_type=jnp.float32
    ).astype(jnp.bfloat16)
    summed = (
        lax.psum_scatter(partial_value, ("split", "pair"), scatter_dimension=2, tiled=True)
        .astype(jnp.float32)
        .astype(jnp.bfloat16)
    )
    narrow = summed.shape[2]
    returning = jnp.swapaxes(summed.reshape(experts_here, n_expert, local_tokens, narrow), 0, 1)
    returning = returning.reshape(total_rows, narrow)
    results = lax.all_to_all(returning, "expert", split_axis=0, concat_axis=0, tiled=True)
    mixed = jnp.dot(mixing, results.astype(jnp.float32), precision=lax.Precision.HIGHEST)
    return mixed.astype(jnp.bfloat16)


def solution(mesh):
    placed = (
        P(("groups", "expert"), ("split", "pair")),
        P(("groups", "expert"), None),
        P(("groups", "expert"), None),
        P(),
        P("expert", "pair", None, "split"),
        P("expert", ("split", "pair"), None),
    )
    return jax.shard_map(
        placed_body(mesh),
        mesh=mesh,
        in_specs=placed,
        out_specs=P(("groups", "expert"), ("split", "pair")),
        check_vma=False,
    )
```

```python
import functools
import jax
import jax.numpy as jnp
from jax import lax
from jax.experimental import pallas as pl
from jax.experimental.pallas import tpu as pltpu
from jax.sharding import PartitionSpec as P

MESH = pl.DeviceIdType.MESH
LANES = 128


def fused(
    n_expert, chunks,
    tokens_hbm, routes_hbm, combine_hbm, home_hbm, gate_up_hbm, down_hbm, out_ref,
    routes_ref, combine_ref, home_ref, own, tok, spread, xi, wbuf, dbuf, mine, pre_out, pre_in, part_out, part_in, kept, stage, fin, mixbuf,
    load_sem, w_sem, d_sem, tok_send, tok_recv, pre_send, pre_recv, part_send, part_recv, fin_send, fin_recv,
):
    groups, expert = lax.axis_index("groups"), lax.axis_index("expert")
    split, pair = lax.axis_index("split"), lax.axis_index("pair")
    partner = (groups, expert, split, 1 - pair)
    rows, narrow = tokens_hbm.shape
    depth = gate_up_hbm.shape[1]
    half = gate_up_hbm.shape[3] // 2
    blocks = half // LANES
    all_rows = n_expert * rows

    load = pltpu.make_async_copy(tokens_hbm, own, load_sem.at[0])
    load.start()
    tables = [
        pltpu.make_async_copy(routes_hbm, routes_ref, load_sem.at[1]),
        pltpu.make_async_copy(combine_hbm, combine_ref, load_sem.at[2]),
        pltpu.make_async_copy(home_hbm, home_ref, load_sem.at[3]),
    ]
    for table in tables:
        table.start()
    step = depth // chunks
    w_loads = []
    for h in range(2):
        at = pl.multiple_of(lax.rem(1 - pair + h, 2) * half, LANES)
        for c in range(chunks):
            w_loads.append(pltpu.make_async_copy(
                gate_up_hbm.at[0, pl.ds(c * step, step), :, pl.ds(at, half)],
                wbuf.at[h, pl.ds(c * step, step)], w_sem.at[h, c]))
            w_loads[-1].start()
    d_loads = []
    for h in range(2):
        core = lax.rem(1 - pair + h, 2)
        for s in range(2):
            at = pl.multiple_of((2 * s + core) * narrow, LANES)
            d_loads.append(pltpu.make_async_copy(
                down_hbm.at[0, :, pl.ds(at, narrow)],
                dbuf.at[h, :, pl.ds(s * narrow, narrow)], d_sem.at[h, s]))
            d_loads[-1].start()

    barrier = pltpu.get_barrier_semaphore()
    for de in range(n_expert):
        for ds in range(2):
            for dp in range(2):
                if de + ds + dp:
                    pl.semaphore_signal(barrier, inc=1, device_id=(
                        groups, lax.rem(expert + de, n_expert), lax.rem(split + ds, 2), lax.rem(pair + dp, 2)),
                        device_id_type=MESH)

    load.wait()
    pl.semaphore_wait(barrier, 4 * n_expert - 1)

    def tok_copy(de, ds):
        return pltpu.make_async_remote_copy(
            src_ref=own, dst_ref=tok.at[de, pair], send_sem=tok_send.at[de, ds], recv_sem=tok_recv.at[de, pair],
            device_id=(groups, lax.rem(expert + de, n_expert), lax.rem(split + ds, 2), split), device_id_type=MESH)

    local = pltpu.make_async_copy(own, tok.at[0, pair], tok_recv.at[0, pair])
    order = sorted(range(n_expert), key=lambda de: -min(de, n_expert - de))
    for de in order:
        for ds in (1, 0):
            if de or ds:
                tok_copy(de, ds).start()

    @pl.when(pair == split)
    def _():
        local.start()

    @pl.when(pair != split)
    def _():
        tok_copy(0, 0).start()

    for table in tables:
        table.wait()
    experts_all = home_ref.shape[0]
    chosen_count = routes_ref.shape[0]
    square = (rows, rows)
    diagonal = lax.broadcasted_iota(jnp.int32, square, 0) == lax.broadcasted_iota(jnp.int32, square, 1)
    slot_rows = jnp.zeros((chosen_count, rows), jnp.int32)
    for e in range(experts_all):
        slot_rows = jnp.where(routes_ref[...] == e, home_ref[e], slot_rows)
    for e in range(n_expert):
        weight = jnp.sum(jnp.where(slot_rows == e, combine_ref[...], 0.0), axis=0, keepdims=True)
        column = jnp.sum(jnp.where(diagonal, jnp.broadcast_to(weight, square), 0.0), axis=1, keepdims=True)
        mixbuf[e] = jnp.broadcast_to(column, (rows, LANES))
    shape = (LANES, 4 * LANES)
    source = lax.broadcasted_iota(jnp.int32, shape, 0)
    place = lax.broadcasted_iota(jnp.int32, shape, 1)
    wanted = jnp.where(place < 2 * LANES, 2 * source, 2 * source + 2 * LANES + 1)
    spread[...] = jnp.where(place == wanted, 1.0, 0.0).astype(jnp.bfloat16)

    for w_load in w_loads:
        w_load.wait()
    for de in range(n_expert):
        for h in range(2):
            pltpu.make_async_copy(own, tok.at[de, h], tok_recv.at[de, h]).wait()

    pieces = []
    for h in range(2):
        whole = jnp.concatenate([tok[de, h].astype(jnp.float32) for de in range(n_expert)], axis=0)
        for c in range(narrow // LANES):
            pieces.append(whole[:, c * LANES:(c + 1) * LANES])
    stacked = jnp.concatenate(pieces, axis=0).astype(jnp.bfloat16)
    wide = jnp.dot(stacked, spread[...], preferred_element_type=jnp.float32).astype(jnp.bfloat16)
    for c in range(len(pieces)):
        at = c * 2 * LANES
        xi[0:all_rows, at:at + 2 * LANES] = wide[c * all_rows:(c + 1) * all_rows, 0:2 * LANES]
        xi[all_rows:, at:at + 2 * LANES] = wide[c * all_rows:(c + 1) * all_rows, 2 * LANES:]

    def weights(number):
        h, j = number // blocks, number % blocks
        return wbuf[h, :, :, j * LANES:(j + 1) * LANES].reshape(2 * depth, LANES)

    def pre_copy(k):
        at = (0, 2 * (blocks // 2) * LANES, half)
        cols = pl.ds(at[k], at[k + 1] - at[k])
        return pltpu.make_async_remote_copy(
            src_ref=pre_out.at[:, cols], dst_ref=pre_in.at[:, cols], send_sem=pre_send.at[k],
            recv_sem=pre_recv.at[k], device_id=partner, device_id_type=MESH)

    pre_copies = [pre_copy(0)] + ([pre_copy(1)] if blocks % 2 else [])
    for n in range(blocks):
        numbers = (2 * n, 2 * n + 1)
        w = jnp.concatenate([weights(k) for k in numbers], axis=1)
        value = jnp.dot(xi[...], w, preferred_element_type=jnp.float32)
        for i, k in enumerate(numbers):
            piece = value[:, i * LANES:(i + 1) * LANES]
            if k < blocks:
                pre_out[:, k * LANES:(k + 1) * LANES] = piece.astype(jnp.bfloat16)
            else:
                mine[:, (k - blocks) * LANES:(k - blocks + 1) * LANES] = piece
        if n == blocks // 2 - 1:
            pre_copies[0].start()
        if blocks % 2 and n == blocks // 2:
            pre_copies[1].start()

    for copy in pre_copies:
        copy.wait_recv()
    total = mine[...] + pre_in[...].astype(jnp.float32)
    gate, up = total[0:all_rows], total[all_rows:]
    hidden = (gate / (1.0 + jnp.exp(-gate)) * up).astype(jnp.bfloat16)

    for d_load in d_loads:
        d_load.wait()
    part_out[...] = jnp.dot(hidden, dbuf[0], preferred_element_type=jnp.float32).astype(jnp.bfloat16)
    part = pltpu.make_async_remote_copy(
        src_ref=part_out, dst_ref=part_in, send_sem=part_send, recv_sem=part_recv,
        device_id=partner, device_id_type=MESH)
    part.start()
    kept[...] = jnp.dot(hidden, dbuf[1], preferred_element_type=jnp.float32)
    part.wait_recv()

    def fin_copy(de, ds):
        return pltpu.make_async_remote_copy(
            src_ref=stage.at[lax.rem(split + ds, 2), de], dst_ref=fin.at[de, ds],
            send_sem=fin_send.at[de, ds], recv_sem=fin_recv.at[de, ds],
            device_id=(groups, lax.rem(expert + de, n_expert), lax.rem(split + ds, 2), pair), device_id_type=MESH)

    for de in order:
        block = (n_expert - de) % n_expert
        for s in range(2):
            at = slice(s * narrow, (s + 1) * narrow)
            lines = slice(block * rows, (block + 1) * rows)
            stage[s, de] = (kept[lines, at] + part_in[:, at].astype(jnp.float32)[lines]).astype(jnp.bfloat16)
        for ds in (1, 0):
            if de or ds:
                fin_copy(de, ds).start()

    result = jnp.zeros((rows, narrow), jnp.float32)
    for de in reversed(order):
        source = lax.rem(expert + n_expert - de, n_expert)
        pair_sum = jnp.zeros((rows, narrow), jnp.float32)
        for ds in range(2):
            if de or ds:
                fin_copy(de, ds).wait_recv()
                pair_sum += fin[de, ds].astype(jnp.float32)
            else:
                pair_sum += stage[split, 0].astype(jnp.float32)
        result += mixbuf[source][:, 0:1] * pair_sum
    out_ref[...] = result.astype(out_ref.dtype)

    for de in range(n_expert):
        for ds in range(2):
            if de or ds:
                tok_copy(de, ds).wait_send()
                fin_copy(de, ds).wait_send()

    @pl.when(pair != split)
    def _():
        tok_copy(0, 0).wait_send()

    for copy in pre_copies:
        copy.wait_send()
    part.wait_send()


def fused_shards(tokens, routes, combine, home, gate_up, down):
    n_expert = lax.axis_size("expert")
    rows, narrow = tokens.shape
    depth, width = gate_up.shape[1], gate_up.shape[3]
    half = width // 2
    all_rows = n_expert * rows
    bf16, f32 = jnp.bfloat16, jnp.float32
    chunks = 4 if depth % 64 == 0 else 1
    in_hbm = pl.BlockSpec(memory_space=pltpu.HBM)
    dma = pltpu.SemaphoreType.DMA
    return pl.pallas_call(
        functools.partial(fused, n_expert, chunks),
        out_shape=jax.ShapeDtypeStruct((rows, narrow), bf16),
        in_specs=[in_hbm] * 6,
        out_specs=pl.BlockSpec(memory_space=pltpu.VMEM),
        scratch_shapes=[
            pltpu.VMEM(routes.shape[::-1], jnp.int32),
            pltpu.VMEM(combine.shape[::-1], f32),
            pltpu.SMEM(home.shape, jnp.int32),
            pltpu.VMEM((rows, narrow), bf16),
            pltpu.VMEM((n_expert, 2, rows, narrow), bf16),
            pltpu.VMEM((LANES, 4 * LANES), bf16),
            pltpu.VMEM((2 * all_rows, 2 * depth), bf16),
            pltpu.VMEM((2, depth, 2, half), bf16),
            pltpu.VMEM((2, down.shape[1], 2 * narrow), bf16),
            pltpu.VMEM((2 * all_rows, half), f32),
            pltpu.VMEM((2 * all_rows, half), bf16),
            pltpu.VMEM((2 * all_rows, half), bf16),
            pltpu.VMEM((all_rows, 2 * narrow), bf16),
            pltpu.VMEM((all_rows, 2 * narrow), bf16),
            pltpu.VMEM((all_rows, 2 * narrow), f32),
            pltpu.VMEM((2, n_expert, rows, narrow), bf16),
            pltpu.VMEM((n_expert, 2, rows, narrow), bf16),
            pltpu.VMEM((n_expert, rows, LANES), f32),
            dma((4,)), dma((2, chunks)), dma((2, 2)),
            dma((n_expert, 2)), dma((n_expert, 2)), dma((2,)), dma((2,)), dma, dma,
            dma((n_expert, 2)), dma((n_expert, 2)),
        ],
        compiler_params=pltpu.CompilerParams(
            collective_id=0, has_side_effects=True, vmem_limit_bytes=40 * 2**20),
    )(*[pltpu.with_memory_space_constraint(x, pltpu.HBM)
        for x in (tokens, routes.T, combine.T, home, gate_up, down)])


def fits(mesh):
    return mesh.shape["split"] == 2 and mesh.shape["pair"] == 2


def placed_body(mesh):
    def body(tokens, routes, combine, home, gate_up, down):
        aligned = (
            tokens.shape[0] == 8 and tokens.shape[1] % LANES == 0 and gate_up.shape[0] == 1
            and gate_up.shape[3] % (2 * LANES) == 0 and home.shape[0] == mesh.shape["expert"]
        )
        chosen = fused_shards if fits(mesh) and aligned else shards
        return chosen(tokens, routes, combine, home, gate_up, down)

    return body


def shards(tokens, routes, combine, home, gate_up, down):
    n_expert = lax.axis_size("expert")
    local_tokens = tokens.shape[0]
    chosen_count = routes.shape[1]
    experts_all = home.shape[0]
    experts_here = gate_up.shape[0]
    total_rows = experts_all * local_tokens
    width = gate_up.shape[1] * 2
    table_ids = jnp.arange(experts_all, dtype=jnp.int32)
    slot = jnp.sum(
        jnp.where(routes[:, :, None] == table_ids[None, None, :], home[None, None, :], 0), axis=-1
    )
    flat_slot = slot.reshape(-1)
    entries = flat_slot.shape[0]
    order_ids = jnp.arange(entries, dtype=jnp.int32)
    earlier = (flat_slot[:, None] == flat_slot[None, :]) & (order_ids[None, :] < order_ids[:, None])
    position = jnp.sum(earlier.astype(jnp.int32), axis=1)
    target = (flat_slot * local_tokens + position).reshape(local_tokens, chosen_count)
    row_ids = jnp.arange(total_rows, dtype=jnp.int32)
    hits = target[None, :, :] == row_ids[:, None, None]
    placing = jnp.sum(hits.astype(jnp.int32), axis=-1).astype(jnp.bfloat16)
    mixing = jnp.sum(jnp.where(hits, combine[None, :, :], jnp.float32(0.0)), axis=-1).T
    outgoing = jnp.dot(placing, tokens, preferred_element_type=jnp.float32).astype(jnp.bfloat16)
    arrived = lax.all_to_all(outgoing, "expert", split_axis=0, concat_axis=0, tiled=True)
    gathered = lax.all_gather(arrived, ("split", "pair"), axis=1, tiled=True)
    rows_each = n_expert * local_tokens
    inputs = gathered.reshape(n_expert, experts_here, local_tokens, width)
    inputs = jnp.swapaxes(inputs, 0, 1).reshape(experts_here, rows_each, width)
    pair_index = lax.axis_index("pair")
    half_width = gate_up.shape[1]
    own_half = lax.dynamic_slice_in_dim(inputs, pair_index * half_width, half_width, 2)
    before = jnp.einsum("erd,edgf->ergf", own_half, gate_up, preferred_element_type=jnp.float32)
    before = lax.psum_scatter(
        before.astype(jnp.bfloat16), "pair", scatter_dimension=3, tiled=True
    ).astype(jnp.float32)
    hidden = (jax.nn.silu(before[:, :, 0, :]) * before[:, :, 1, :]).astype(jnp.bfloat16)
    partial_value = jnp.einsum(
        "erf,efd->erd", hidden, down, preferred_element_type=jnp.float32
    ).astype(jnp.bfloat16)
    summed = (
        lax.psum_scatter(partial_value, ("split", "pair"), scatter_dimension=2, tiled=True)
        .astype(jnp.float32)
        .astype(jnp.bfloat16)
    )
    narrow = summed.shape[2]
    returning = jnp.swapaxes(summed.reshape(experts_here, n_expert, local_tokens, narrow), 0, 1)
    returning = returning.reshape(total_rows, narrow)
    results = lax.all_to_all(returning, "expert", split_axis=0, concat_axis=0, tiled=True)
    mixed = jnp.dot(mixing, results.astype(jnp.float32), precision=lax.Precision.HIGHEST)
    return mixed.astype(jnp.bfloat16)


def solution(mesh):
    placed = (
        P(("groups", "expert"), ("split", "pair")),
        P(("groups", "expert"), None),
        P(("groups", "expert"), None),
        P(),
        P("expert", "pair", None, "split"),
        P("expert", ("split", "pair"), None),
    )
    return jax.shard_map(
        placed_body(mesh),
        mesh=mesh,
        in_specs=placed,
        out_specs=P(("groups", "expert"), ("split", "pair")),
        check_vma=False,
    )
```
